256 devices in a mesh: site: 2 (over z_hi), row: 4 (over z_lo), col: 32 (over y, x, core).
Axes of the slice: x: 4, y: 4, z: 8 (z_hi: 2, z_lo: 4; z = z_hi * 4 + z_lo), core: 2. Of those that a mesh axis runs over, the one named last changes fastest.
Arguments:
- pair_array: bfloat16 [1024, 512, 128], P(('site', 'row'), 'col'), parts along dimension 0, may hold values from -6 to 6
- in_gain: float32 [128], replicated, may hold values from 0.25 to 1.75
- left_weight: bfloat16 [256, 128], P('site'), parts along dimension 0, may hold values from -0.5 to 0.5
- right_weight: bfloat16 [256, 128], P('site'), parts along dimension 0, may hold values from -0.5 to 0.5
- mid_gain: float32 [128], replicated, may hold values from 0.25 to 1.75
- out_weight: bfloat16 [256, 128], P('site'), parts along dimension 0, may hold values from -0.5 to 0.5
- out_gate: bfloat16 [256, 128], P('site'), parts along dimension 0, may hold values from -0.5 to 0.5
Outputs:
- triangle_out: bfloat16 [1024, 512, 128], P(('site', 'row'), 'col'), parts along dimension 0
The draws below stay inside these ranges and needn't reach their ends.
There are 2 independent parts, one for each index of `site`. The reference program is written for one: setup_inputs(seed, part) draws one part's arguments, and reference() takes and returns one part's arrays. A program takes and returns all parts, laid end to end along the dimension named above; an argument that names none is the same for every part. Nothing has to cross between parts.
All inputs are finite; a program needn't handle non-finite values.
Results may differ from the reference program's by a relative error of at most 0.012.
Values may be sent and summed in bfloat16 or wider, within the bound.
No kernel may reach another device: no remote copies, remote signals or barrier semaphores. Data moves between devices by JAX's collectives and lax.ppermute only.
A program may use at most 64 MiB of HBM per device.

```python
import jax
import jax.numpy as jnp
from jax import lax

RESIDUES = 512
PAIR_WIDTH = 128
MIX_WIDTH = 128


def block_levels(rng, extent, cuts, low, high):
    loudness = 1.0
    for dim, blocks in cuts:
        steps = jax.random.uniform(jax.random.fold_in(jax.random.fold_in(rng, 6), dim), (blocks,), jnp.float32, low / len(cuts), high / len(cuts))
        loudness = loudness * jnp.repeat(jnp.exp(steps), extent[dim] // blocks).reshape((-1,) + (1,) * (len(extent) - 1 - dim))
    return loudness


def scatter_about(key, extent, spread, reach, pieces=(), held_as=jnp.bfloat16):
    drawn = jax.random.normal(key, extent, jnp.float32) * spread
    if len(pieces) > 0:
        drawn = block_levels(key, extent, pieces, -0.22, 0.18) * drawn
    return jnp.clip(drawn, min=-reach, max=reach).astype(held_as)


def setup_inputs(seed: int = 0, part: int = 0) -> dict:
    keys = jax.random.split(jax.random.key(seed), 8)
    part_keys = jax.random.split(jax.random.fold_in(keys[7], part), 8)
    return {
        "pair_array": scatter_about(part_keys[0], (RESIDUES, RESIDUES, PAIR_WIDTH), 1.0, 6.0, ((0, 4), (1, 32))),
        "in_gain": jnp.clip(1.0 + 0.15 * jax.random.normal(keys[1], (PAIR_WIDTH,), jnp.float32), 0.25, 1.75),
        "left_weight": scatter_about(part_keys[2], (PAIR_WIDTH, MIX_WIDTH), PAIR_WIDTH ** -0.5, 0.5),
        "right_weight": scatter_about(part_keys[3], (PAIR_WIDTH, MIX_WIDTH), PAIR_WIDTH ** -0.5, 0.5),
        "mid_gain": jnp.clip(1.0 + 0.15 * jax.random.normal(keys[4], (MIX_WIDTH,), jnp.float32), 0.25, 1.75),
        "out_weight": scatter_about(part_keys[5], (MIX_WIDTH, PAIR_WIDTH), MIX_WIDTH ** -0.5, 0.5),
        "out_gate": scatter_about(part_keys[6], (PAIR_WIDTH, PAIR_WIDTH), PAIR_WIDTH ** -0.5, 0.5),
    }


def norm_channels(values, channel_gain):
    centred = values - lax.optimization_barrier(jnp.mean(values, axis=-1, keepdims=True))
    return centred * lax.rsqrt(lax.optimization_barrier(jnp.mean(centred * centred, axis=-1, keepdims=True)) + 1e-05) * channel_gain

def both_factors(pair_in, in_gain, left_weight, right_weight):
    ready = norm_channels(pair_in.astype(jnp.float32), in_gain).astype(jnp.bfloat16)
    ready = lax.optimization_barrier(ready)
    left = jnp.einsum('ijc,cd->ijd', ready.astype(jnp.float32), left_weight.astype(jnp.float32))
    right = jnp.einsum('ijc,cd->ijd', ready.astype(jnp.float32), right_weight.astype(jnp.float32))
    return (ready, left.astype(jnp.bfloat16), right.astype(jnp.bfloat16))

def finish_pair(mixed, ready, mid_gain, out_weight, out_gate):
    scaled = norm_channels(mixed.astype(jnp.float32), mid_gain).astype(jnp.bfloat16)
    scaled = lax.optimization_barrier(scaled)
    gate = jax.nn.sigmoid(jnp.einsum('ijc,cd->ijd', ready.astype(jnp.float32), out_gate.astype(jnp.float32)))
    return (jnp.einsum('ijd,dc->ijc', scaled.astype(jnp.float32), out_weight.astype(jnp.float32)) * gate).astype(jnp.bfloat16)

def reference(pair_array, in_gain, left_weight, right_weight, mid_gain, out_weight, out_gate):
    ready, left, right = both_factors(pair_array, in_gain, left_weight, right_weight)
    left, right = lax.optimization_barrier((left, right))

    def one_channel(pair_of):
        return (jnp.dot(pair_of[0].T, pair_of[1], preferred_element_type=jnp.float32) * RESIDUES ** (-0.5)).astype(jnp.bfloat16)
    mixed = jnp.moveaxis(lax.map(one_channel, (jnp.moveaxis(left, -1, 0), jnp.moveaxis(right, -1, 0))), 0, -1)
    mixed = lax.optimization_barrier(mixed)
    return finish_pair(mixed, ready, mid_gain, out_weight, out_gate)
```

```python
import functools

import jax
import jax.numpy as jnp
from jax import lax
from jax.experimental import pallas as pl
from jax.experimental.pallas import tpu as pltpu
from jax.sharding import PartitionSpec as P

VMEM = pl.BlockSpec(memory_space=pltpu.VMEM)
F32 = jnp.float32
BF16 = jnp.bfloat16


def front_kernel(x_ref, gain_ref, wl_ref, wr_ref, ready_ref, out_ref, rows_ref, tiles_ref):
    k, n, c = x_ref.shape
    d = wl_ref.shape[1]
    step = 16
    gain = gain_ref[...]

    def norm(s, _):
        x = x_ref[pl.ds(s * step, step)].reshape(step * n, c).astype(F32)
        centred = x - jnp.mean(x, axis=-1, keepdims=True)
        power = jnp.mean(centred * centred, axis=-1, keepdims=True)
        ready = (centred * lax.rsqrt(power + 1e-05) * gain).astype(BF16)
        ready_ref[pl.ds(s * step * n, step * n), :] = ready
        rows_ref[pl.ds(s * step * n, step * n), :] = ready.astype(F32)
        return 0

    lax.fori_loop(0, k // step, norm, 0)
    wl = wl_ref[...].astype(F32).T.astype(BF16)
    wr = wr_ref[...].astype(F32).T.astype(BF16)
    for i in range(n):
        ready = rows_ref[pl.ds(i, k, stride=n), :].astype(BF16)
        for side, w in ((0, wl), (1, wr)):
            tiles_ref[pl.ds(side * n + i, d, stride=2 * n), :] = lax.dot_general(
                w, ready, (((1,), (1,)), ((), ())), preferred_element_type=F32
            )

    def store(s, _):
        t = tiles_ref[pl.ds(s * 256, 256), :].astype(BF16)
        out_ref[pl.ds(s * (256 // (2 * n)), 256 // (2 * n))] = t.reshape(256 // (2 * n), 2 * n, k)
        return 0

    lax.fori_loop(0, d * 2 * n // 256, store, 0)


def middle_kernel(rows, scale, in_ref, out_ref):
    parts, n2, k = in_ref.shape
    n = n2 // 2
    cols = parts // rows
    for to in range(rows):
        total = jnp.zeros((cols * n, k), F32)
        for r in range(rows):
            left = in_ref[pl.ds(r * cols + to * (cols // rows), cols // rows), :n, :].reshape(cols // rows * n, k)
            right = in_ref[pl.ds(r * cols, cols), n:, :].reshape(cols * n, k)
            total += lax.dot_general(right, left, (((1,), (1,)), ((), ())), preferred_element_type=F32)
        out_ref[pl.ds(to * cols, cols)] = (total * scale).astype(BF16).reshape(cols, n, k)


def back_kernel(m_ref, ready_ref, gain_ref, w_ref, gate_ref, out_ref, rows_ref, sums_ref):
    d, n, k = m_ref.shape
    c = w_ref.shape[1]
    step = 8

    def total(s, acc):
        return acc + jnp.sum(m_ref[pl.ds(s * step, step)].astype(F32), axis=0)

    mean = lax.fori_loop(0, d // step, total, jnp.zeros((n, k), F32)) * (1.0 / d)

    def squares(s, acc):
        centred = m_ref[pl.ds(s * step, step)].astype(F32) - mean
        return acc + jnp.sum(centred * centred, axis=0)

    power = lax.fori_loop(0, d // step, squares, jnp.zeros((n, k), F32)) * (1.0 / d)
    root = lax.rsqrt(power + 1e-05)

    def scaled(s, _):
        centred = m_ref[pl.ds(s * step, step)].astype(F32) - mean
        rows_ref[pl.ds(s * step, step)] = centred * root
        return 0

    lax.fori_loop(0, d // step, scaled, 0)
    gain = gain_ref[...]
    w = w_ref[...]
    flat = rows_ref.reshape(d * n, k)
    for j in range(n):
        t = (flat[pl.ds(j, d, stride=n), :].T * gain).astype(BF16)
        sums_ref[pl.ds(j, k, stride=n), :] = jnp.dot(t, w, preferred_element_type=F32)
    g = gate_ref[...]

    def finish(s, _):
        at = pl.ds(s * 16 * n, 16 * n)
        gate = jax.nn.sigmoid(jnp.dot(ready_ref[at, :], g, preferred_element_type=F32))
        out_ref[pl.ds(s * 16, 16)] = (sums_ref[at, :] * gate).astype(BF16).reshape(16, n, c)
        return 0

    lax.fori_loop(0, k // 16, finish, 0)


def body(pair_array, in_gain, left_weight, right_weight, mid_gain, out_weight, out_gate):
    k, n, c = pair_array.shape
    d = left_weight.shape[1]
    rows, cols = lax.axis_size("row"), lax.axis_size("col")
    params = pltpu.CompilerParams(vmem_limit_bytes=32 << 20)
    ready, factors = pl.pallas_call(
        front_kernel,
        out_shape=(
            jax.ShapeDtypeStruct((k * n, c), BF16),
            jax.ShapeDtypeStruct((d, 2 * n, k), BF16),
        ),
        in_specs=[VMEM] * 4,
        out_specs=(VMEM, VMEM),
        scratch_shapes=[pltpu.VMEM((k * n, c), F32), pltpu.VMEM((d * 2 * n, k), F32)],
        compiler_params=params,
        name="front",
    )(pair_array, in_gain.reshape(1, c), left_weight, right_weight)
    factors = lax.all_to_all(factors, ("row", "col"), split_axis=0, concat_axis=0, tiled=True)
    mixed = pl.pallas_call(
        functools.partial(middle_kernel, rows, (k * rows) ** -0.5),
        out_shape=jax.ShapeDtypeStruct((rows * cols, n, k), BF16),
        in_specs=[VMEM],
        out_specs=VMEM,
        compiler_params=params,
        name="middle",
    )(factors)
    mixed = lax.all_to_all(mixed, ("row", "col"), split_axis=0, concat_axis=0, tiled=True)
    return pl.pallas_call(
        back_kernel,
        out_shape=jax.ShapeDtypeStruct((k, n, c), BF16),
        in_specs=[VMEM] * 5,
        out_specs=VMEM,
        scratch_shapes=[pltpu.VMEM((d, n, k), F32), pltpu.VMEM((k * n, c), F32)],
        compiler_params=params,
        name="back",
    )(mixed, ready, mid_gain.reshape(1, d), out_weight, out_gate)


def solution(mesh):
    return jax.shard_map(
        body,
        mesh=mesh,
        in_specs=(
            P(("site", "row"), "col", None),
            P(),
            P("site", None),
            P("site", None),
            P(),
            P("site", None),
            P("site", None),
        ),
        out_specs=P(("site", "row"), "col", None),
        check_vma=False,
    )
```

```python
import functools

import jax
import jax.numpy as jnp
from jax import lax
from jax.experimental import pallas as pl
from jax.experimental.pallas import tpu as pltpu
from jax.sharding import PartitionSpec as P

VMEM = pl.BlockSpec(memory_space=pltpu.VMEM)
HBM = pl.BlockSpec(memory_space=pltpu.HBM)
F32 = jnp.float32
BF16 = jnp.bfloat16
PIECES = 2


def nt(a, b):
    return lax.dot_general(a, b, (((1,), (1,)), ((), ())), preferred_element_type=F32)


def in_hbm(x):
    return pltpu.with_memory_space_constraint(x, pltpu.HBM)


def front_kernel(x_hbm, gain_hbm, wl_hbm, wr_hbm, ready_ref, out_ref,
                 x_ref, gain_ref, wl_ref, wr_ref, rows_ref, tiles_ref, sems):
    k, n, c = x_ref.shape
    d = wl_ref.shape[1]
    pitch, wide = n + 1, 2 * n + 1
    part = k // PIECES
    pieces = [
        pltpu.make_async_copy(x_hbm.at[pl.ds(p * part, part)], x_ref.at[pl.ds(p * part, part)], sems.at[p])
        for p in range(PIECES)
    ]
    weights = [
        pltpu.make_async_copy(gain_hbm, gain_ref, sems.at[PIECES]),
        pltpu.make_async_copy(wl_hbm, wl_ref, sems.at[PIECES + 1]),
        pltpu.make_async_copy(wr_hbm, wr_ref, sems.at[PIECES + 2]),
    ]
    for copy in weights[:1] + pieces + weights[1:]:
        copy.start()
    weights[0].wait()
    gain = gain_ref[...]
    for p in range(PIECES):
        pieces[p].wait()
        x = x_ref[pl.ds(p * part, part)].reshape(part * n, c).astype(F32)
        centred = x - jnp.mean(x, axis=-1, keepdims=True)
        power = jnp.mean(centred * centred, axis=-1, keepdims=True)
        ready = (centred * lax.rsqrt(power + 1e-05) * gain).astype(BF16)
        ready_ref[pl.ds(p * part * n, part * n), :] = ready
        rows = ready.astype(F32)
        for q in range(part):
            rows_ref[pl.ds((p * part + q) * pitch, n), :] = rows[q * n : (q + 1) * n]
    weights[1].wait()
    weights[2].wait()
    w = jnp.concatenate([wl_ref[...].astype(F32).T, wr_ref[...].astype(F32).T], axis=0).astype(BF16)
    for i in range(n):
        both = nt(w, rows_ref[pl.ds(i, k, stride=pitch), :].astype(BF16))
        tiles_ref[pl.ds(i, d, stride=wide), :] = both[:d]
        tiles_ref[pl.ds(n + i, d, stride=wide), :] = both[d:]
    step = 32

    def store(s, _):
        for q in range(step):
            out_ref[s * step + q] = tiles_ref[pl.ds((s * step + q) * wide, 2 * n), :].astype(BF16)
        return 0

    lax.fori_loop(0, d // step, store, 0)


def gate_kernel(ready_ref, gate_hbm, gain_hbm, w_hbm, out_ref, gain_out_ref, w_out_ref, gate_ref, gain_ref, sems):
    copies = [
        pltpu.make_async_copy(gate_hbm, gate_ref, sems.at[0]),
        pltpu.make_async_copy(gain_hbm, gain_ref, sems.at[1]),
        pltpu.make_async_copy(w_hbm, w_out_ref, sems.at[2]),
    ]
    for copy in copies:
        copy.start()
    for copy in copies:
        copy.wait()
    g = gate_ref[...]
    step = 256

    def one(s, _):
        at = pl.ds(s * step, step)
        out_ref[at, :] = jax.nn.sigmoid(jnp.dot(ready_ref[at, :], g, preferred_element_type=F32))
        return 0

    lax.fori_loop(0, ready_ref.shape[0] // step, one, 0)
    gain_out_ref[...] = gain_ref[...]


def middle_kernel(rows, scale, in_ref, out_ref):
    parts, n2, k = in_ref.shape
    n = n2 // 2
    cols = parts // rows
    few = cols // rows
    right = jnp.concatenate([in_ref[pl.ds(r * cols, cols), n:, :].reshape(cols * n, k) for r in range(rows)], axis=1)
    for to in range(rows):
        left = jnp.concatenate(
            [
                in_ref[pl.ds(r * cols + to * few, few), :n, :].reshape(few * n, k).astype(F32).T.astype(BF16)
                for r in range(rows)
            ],
            axis=0,
        )
        total = jnp.dot(right, left, preferred_element_type=F32) * scale
        out_ref[pl.ds(to * cols, cols)] = total.astype(BF16).reshape(cols, n, k)


def back_kernel(m_ref, gate_ref, gain_ref, w_ref, out_hbm, rows_ref, sums_ref, out_ref, sems):
    d, n, k = m_ref.shape
    pitch = n + 1
    step = 32

    def total(s, acc):
        return acc + jnp.sum(m_ref[pl.ds(s * step, step)].astype(F32), axis=0)

    mean = lax.fori_loop(0, d // step, total, jnp.zeros((n, k), F32)) * (1.0 / d)

    def squares(s, acc):
        centred = m_ref[pl.ds(s * step, step)].astype(F32) - mean
        return acc + jnp.sum(centred * centred, axis=0)

    power = lax.fori_loop(0, d // step, squares, jnp.zeros((n, k), F32)) * (1.0 / d)
    root = lax.rsqrt(power + 1e-05)

    def scaled(s, _):
        for q in range(step):
            centred = m_ref[s * step + q].astype(F32) - mean
            rows_ref[pl.ds((s * step + q) * pitch, n), :] = centred * root
        return 0

    lax.fori_loop(0, d // step, scaled, 0)
    w = w_ref[...]
    gain = gain_ref[...]
    for j in range(n):
        t = (rows_ref[pl.ds(j, d, stride=pitch), :].T * gain).astype(BF16)
        sums_ref[pl.ds(j, k, stride=pitch), :] = jnp.dot(t, w, preferred_element_type=F32)
    part = k // PIECES
    copies = []
    for p in range(PIECES):

        def finish(s, _):
            for q in range(step):
                at = p * part + s * step + q
                out_ref[at] = (sums_ref[pl.ds(at * pitch, n), :] * gate_ref[pl.ds(at * n, n), :]).astype(BF16)
            return 0

        lax.fori_loop(0, part // step, finish, 0)
        copy = pltpu.make_async_copy(
            out_ref.at[pl.ds(p * part, part)], out_hbm.at[pl.ds(p * part, part)], sems.at[p]
        )
        copy.start()
        copies.append(copy)
    for copy in copies:
        copy.wait()


def body(pair_array, in_gain, left_weight, right_weight, mid_gain, out_weight, out_gate):
    k, n, c = pair_array.shape
    d = left_weight.shape[1]
    rows, cols = lax.axis_size("row"), lax.axis_size("col")
    params = pltpu.CompilerParams(vmem_limit_bytes=32 << 20)
    ready, factors = pl.pallas_call(
        front_kernel,
        out_shape=(
            jax.ShapeDtypeStruct((k * n, c), BF16),
            jax.ShapeDtypeStruct((d, 2 * n, k), BF16),
        ),
        in_specs=[HBM] * 4,
        out_specs=(VMEM, VMEM),
        scratch_shapes=[
            pltpu.VMEM((k, n, c), BF16),
            pltpu.VMEM((1, c), F32),
            pltpu.VMEM((c, d), BF16),
            pltpu.VMEM((c, d), BF16),
            pltpu.VMEM((k * (n + 1), c), F32),
            pltpu.VMEM((d * (2 * n + 1), k), F32),
            pltpu.SemaphoreType.DMA((PIECES + 3,)),
        ],
        compiler_params=params,
        name="front",
    )(in_hbm(pair_array), in_hbm(in_gain.reshape(1, c)), in_hbm(left_weight), in_hbm(right_weight))
    factors = lax.all_to_all(factors, ("row", "col"), split_axis=0, concat_axis=0, tiled=True)
    gate, gain, weight = pl.pallas_call(
        gate_kernel,
        out_shape=(
            jax.ShapeDtypeStruct((k * n, c), F32),
            jax.ShapeDtypeStruct((1, d), F32),
            jax.ShapeDtypeStruct((d, c), BF16),
        ),
        in_specs=[VMEM, HBM, HBM, HBM],
        out_specs=(VMEM, VMEM, VMEM),
        scratch_shapes=[
            pltpu.VMEM((c, c), BF16),
            pltpu.VMEM((1, d), F32),
            pltpu.SemaphoreType.DMA((3,)),
        ],
        compiler_params=params,
        cost_estimate=pl.CostEstimate(flops=4_000_000_000, bytes_accessed=2 << 20, transcendentals=k * n * c),
        name="gate",
    )(ready, in_hbm(out_gate), in_hbm(mid_gain.reshape(1, d)), in_hbm(out_weight))
    mixed = pl.pallas_call(
        functools.partial(middle_kernel, rows, (k * rows) ** -0.5),
        out_shape=pltpu.VMEM((rows * cols, n, k), BF16),
        in_specs=[VMEM],
        out_specs=VMEM,
        compiler_params=params,
        name="middle",
    )(factors)
    mixed = lax.all_to_all(mixed, ("row", "col"), split_axis=0, concat_axis=0, tiled=True)
    return pl.pallas_call(
        back_kernel,
        out_shape=jax.ShapeDtypeStruct((k, n, c), BF16),
        in_specs=[VMEM] * 4,
        out_specs=HBM,
        scratch_shapes=[
            pltpu.VMEM((d * (n + 1), k), F32),
            pltpu.VMEM((k * (n + 1), c), F32),
            pltpu.VMEM((k, n, c), BF16),
            pltpu.SemaphoreType.DMA((PIECES,)),
        ],
        compiler_params=params,
        name="back",
    )(mixed, gate, gain, weight)


def solution(mesh):
    return jax.shard_map(
        body,
        mesh=mesh,
        in_specs=(
            P(("site", "row"), "col", None),
            P(),
            P("site", None),
            P("site", None),
            P(),
            P("site", None),
            P("site", None),
        ),
        out_specs=P(("site", "row"), "col", None),
        check_vma=False,
    )
```

```python
import functools

import jax
import jax.numpy as jnp
from jax import lax
from jax.experimental import pallas as pl
from jax.experimental.pallas import tpu as pltpu
from jax.sharding import PartitionSpec as P

VMEM = pl.BlockSpec(memory_space=pltpu.VMEM)
HBM = pl.BlockSpec(memory_space=pltpu.HBM)
F32 = jnp.float32
BF16 = jnp.bfloat16
PIECES = 2


def nt(a, b):
    return lax.dot_general(a, b, (((1,), (1,)), ((), ())), preferred_element_type=F32)


def in_hbm(x):
    return pltpu.with_memory_space_constraint(x, pltpu.HBM)


def front_kernel(x_hbm, gain_hbm, wl_hbm, wr_hbm, ready_ref, out_ref,
                 x_ref, gain_ref, wl_ref, wr_ref, rows_ref, tiles_ref, sems):
    k, n, c = x_ref.shape
    d = wl_ref.shape[1]
    pitch, wide = n + 1, 2 * n + 1
    part = k // PIECES
    pieces = [
        pltpu.make_async_copy(x_hbm.at[pl.ds(p * part, part)], x_ref.at[pl.ds(p * part, part)], sems.at[p])
        for p in range(PIECES)
    ]
    weights = [
        pltpu.make_async_copy(gain_hbm, gain_ref, sems.at[PIECES]),
        pltpu.make_async_copy(wl_hbm, wl_ref, sems.at[PIECES + 1]),
        pltpu.make_async_copy(wr_hbm, wr_ref, sems.at[PIECES + 2]),
    ]
    for copy in weights[:1] + pieces + weights[1:]:
        copy.start()
    weights[0].wait()
    gain = gain_ref[...]
    for p in range(PIECES):
        pieces[p].wait()
        x = x_ref[pl.ds(p * part, part)].reshape(part * n, c).astype(F32)
        centred = x - jnp.mean(x, axis=-1, keepdims=True)
        power = jnp.mean(centred * centred, axis=-1, keepdims=True)
        ready = (centred * lax.rsqrt(power + 1e-05) * gain).astype(BF16)
        ready_ref[pl.ds(p * part * n, part * n), :] = ready
        rows = ready.astype(F32)
        for q in range(part):
            rows_ref[pl.ds((p * part + q) * pitch, n), :] = rows[q * n : (q + 1) * n]
    weights[1].wait()
    weights[2].wait()
    w = jnp.concatenate([wl_ref[...].astype(F32).T, wr_ref[...].astype(F32).T], axis=0).astype(BF16)
    for i in range(n):
        both = nt(w, rows_ref[pl.ds(i, k, stride=pitch), :].astype(BF16))
        tiles_ref[pl.ds(i, d, stride=wide), :] = both[:d]
        tiles_ref[pl.ds(n + i, d, stride=wide), :] = both[d:]
    step = 32

    def store(s, _):
        for q in range(step):
            out_ref[s * step + q] = tiles_ref[pl.ds((s * step + q) * wide, 2 * n), :].astype(BF16)
        return 0

    lax.fori_loop(0, d // step, store, 0)


def gate_kernel(ready_ref, gate_hbm, gain_hbm, w_hbm, out_ref, gain_out_ref, w_out_ref, gate_ref, gain_ref, sems):
    copies = [
        pltpu.make_async_copy(gate_hbm, gate_ref, sems.at[0]),
        pltpu.make_async_copy(gain_hbm, gain_ref, sems.at[1]),
        pltpu.make_async_copy(w_hbm, w_out_ref, sems.at[2]),
    ]
    for copy in copies:
        copy.start()
    for copy in copies:
        copy.wait()
    g = gate_ref[...]
    step = 256

    def one(s, _):
        at = pl.ds(s * step, step)
        out_ref[at, :] = jax.nn.sigmoid(jnp.dot(ready_ref[at, :], g, preferred_element_type=F32))
        return 0

    lax.fori_loop(0, ready_ref.shape[0] // step, one, 0)
    gain_out_ref[...] = gain_ref[...]


def middle_kernel(rows, scale, own_ref, other_ref, out_ref):
    chips, two, n, k = other_ref.shape
    per = chips // rows
    few = per // rows
    for dd in range(two):
        right = jnp.concatenate(
            [own_ref[pl.ds(r * per, per), dd, n:, :].reshape(per * n, k) for r in range(rows)], axis=1
        )
        for to in range(rows):
            left = []
            for r in range(rows):
                at = pl.ds(r * per + to * few, few)
                both = jnp.concatenate(
                    [own_ref[at, dd, :n, :].reshape(few * n, k), other_ref[at, dd].reshape(few * n, k)], axis=0
                )
                left.append(both.astype(F32).T.astype(BF16))
            total = jnp.dot(right, jnp.concatenate(left, axis=0), preferred_element_type=F32) * scale
            out_ref[pl.ds(to * per, per), dd] = total.astype(BF16).reshape(per, n, k)


def back_kernel(m_ref, gate_ref, gain_ref, w_ref, out_hbm, rows_ref, sums_ref, out_ref, sems):
    d, n, k = m_ref.shape
    pitch = n + 1
    step = 32

    def total(s, acc):
        return acc + jnp.sum(m_ref[pl.ds(s * step, step)].astype(F32), axis=0)

    mean = lax.fori_loop(0, d // step, total, jnp.zeros((n, k), F32)) * (1.0 / d)

    def squares(s, acc):
        centred = m_ref[pl.ds(s * step, step)].astype(F32) - mean
        return acc + jnp.sum(centred * centred, axis=0)

    power = lax.fori_loop(0, d // step, squares, jnp.zeros((n, k), F32)) * (1.0 / d)
    root = lax.rsqrt(power + 1e-05)

    def scaled(s, _):
        for q in range(step):
            centred = m_ref[s * step + q].astype(F32) - mean
            rows_ref[pl.ds((s * step + q) * pitch, n), :] = centred * root
        return 0

    lax.fori_loop(0, d // step, scaled, 0)
    w = w_ref[...]
    gain = gain_ref[...]
    core = lax.rem(lax.axis_index("col"), 2)
    for j in range(n):
        t = (rows_ref[pl.ds(j, d, stride=pitch), :].T * gain).astype(BF16)
        sums = jnp.dot(t, w, preferred_element_type=F32)
        for h in range(2):
            for q in range(k // (2 * n)):
                at = (2 * q + (1 - core if h else core)) * n * pitch + j
                block = h * (k // 2) + q * n
                sums_ref[pl.ds(at, n, stride=pitch), :] = sums[block : block + n]
    part = k // PIECES
    copies = []
    for p in range(PIECES):

        def finish(s, _):
            for q in range(step):
                at = p * part + s * step + q
                out_ref[at] = (sums_ref[pl.ds(at * pitch, n), :] * gate_ref[pl.ds(at * n, n), :]).astype(BF16)
            return 0

        lax.fori_loop(0, part // step, finish, 0)
        copy = pltpu.make_async_copy(
            out_ref.at[pl.ds(p * part, part)], out_hbm.at[pl.ds(p * part, part)], sems.at[p]
        )
        copy.start()
        copies.append(copy)
    for copy in copies:
        copy.wait()


def body(pair_array, in_gain, left_weight, right_weight, mid_gain, out_weight, out_gate):
    k, n, c = pair_array.shape
    d = left_weight.shape[1]
    rows, cols = lax.axis_size("row"), lax.axis_size("col")
    params = pltpu.CompilerParams(vmem_limit_bytes=32 << 20)
    ready, factors = pl.pallas_call(
        front_kernel,
        out_shape=(
            jax.ShapeDtypeStruct((k * n, c), BF16),
            jax.ShapeDtypeStruct((d, 2 * n, k), BF16),
        ),
        in_specs=[HBM] * 4,
        out_specs=(VMEM, VMEM),
        scratch_shapes=[
            pltpu.VMEM((k, n, c), BF16),
            pltpu.VMEM((1, c), F32),
            pltpu.VMEM((c, d), BF16),
            pltpu.VMEM((c, d), BF16),
            pltpu.VMEM((k * (n + 1), c), F32),
            pltpu.VMEM((d * (2 * n + 1), k), F32),
            pltpu.SemaphoreType.DMA((PIECES + 3,)),
        ],
        compiler_params=params,
        name="front",
    )(in_hbm(pair_array), in_hbm(in_gain.reshape(1, c)), in_hbm(left_weight), in_hbm(right_weight))
    same_core = [[r * cols + q * 2 + core for r in range(rows) for q in range(cols // 2)] for core in range(2)]
    chips = rows * cols // 2

    def exchange(x):
        return lax.all_to_all(
            x, ("row", "col"), split_axis=0, concat_axis=0, tiled=True, axis_index_groups=same_core
        )

    factors = exchange(factors).reshape(chips, 2, 2 * n, k)
    other = lax.ppermute(factors[:, :, :n], "col", [(i, i ^ 1) for i in range(cols)])
    gate, gain, weight = pl.pallas_call(
        gate_kernel,
        out_shape=(
            jax.ShapeDtypeStruct((k * n, c), F32),
            jax.ShapeDtypeStruct((1, d), F32),
            jax.ShapeDtypeStruct((d, c), BF16),
        ),
        in_specs=[VMEM, HBM, HBM, HBM],
        out_specs=(VMEM, VMEM, VMEM),
        scratch_shapes=[
            pltpu.VMEM((c, c), BF16),
            pltpu.VMEM((1, d), F32),
            pltpu.SemaphoreType.DMA((3,)),
        ],
        compiler_params=params,
        cost_estimate=pl.CostEstimate(flops=4_000_000_000, bytes_accessed=2 << 20, transcendentals=k * n * c),
        name="gate",
    )(ready, in_hbm(out_gate), in_hbm(mid_gain.reshape(1, d)), in_hbm(out_weight))
    factors, other, gate, gain, weight = lax.optimization_barrier((factors, other, gate, gain, weight))
    mixed = pl.pallas_call(
        functools.partial(middle_kernel, rows, (k * rows) ** -0.5),
        out_shape=jax.ShapeDtypeStruct((chips, 2, n, k), BF16),
        in_specs=[VMEM] * 2,
        out_specs=VMEM,
        compiler_params=params,
        name="middle",
    )(factors, other)
    mixed = exchange(mixed.reshape(d, n, k))
    return pl.pallas_call(
        back_kernel,
        out_shape=jax.ShapeDtypeStruct((k, n, c), BF16),
        in_specs=[VMEM] * 4,
        out_specs=HBM,
        scratch_shapes=[
            pltpu.VMEM((d * (n + 1), k), F32),
            pltpu.VMEM((k * (n + 1), c), F32),
            pltpu.VMEM((k, n, c), BF16),
            pltpu.SemaphoreType.DMA((PIECES,)),
        ],
        compiler_params=params,
        name="back",
    )(mixed, gate, gain, weight)


def solution(mesh):
    return jax.shard_map(
        body,
        mesh=mesh,
        in_specs=(
            P(("site", "row"), "col", None),
            P(),
            P("site", None),
            P("site", None),
            P(),
            P("site", None),
            P("site", None),
        ),
        out_specs=P(("site", "row"), "col", None),
        check_vma=False,
    )
```

```python
import functools

import jax
import jax.numpy as jnp
from jax import lax
from jax.experimental import pallas as pl
from jax.experimental.pallas import tpu as pltpu
from jax.sharding import PartitionSpec as P

VMEM = pl.BlockSpec(memory_space=pltpu.VMEM)
HBM = pl.BlockSpec(memory_space=pltpu.HBM)
F32 = jnp.float32
BF16 = jnp.bfloat16
PIECES = 2


def nt(a, b):
    return lax.dot_general(a, b, (((1,), (1,)), ((), ())), preferred_element_type=F32)


def in_hbm(x):
    return pltpu.with_memory_space_constraint(x, pltpu.HBM)


def front_kernel(x_hbm, gain_hbm, wl_hbm, wr_hbm, ready_ref, out_ref,
                 x_ref, gain_ref, wl_ref, wr_ref, rows_ref, tiles_ref, sems):
    k, n, c = x_ref.shape
    d = wl_ref.shape[1]
    pitch, wide = n + 1, 2 * n + 1
    part = k // PIECES
    pieces = [
        pltpu.make_async_copy(x_hbm.at[pl.ds(p * part, part)], x_ref.at[pl.ds(p * part, part)], sems.at[p])
        for p in range(PIECES)
    ]
    weights = [
        pltpu.make_async_copy(gain_hbm, gain_ref, sems.at[PIECES]),
        pltpu.make_async_copy(wl_hbm, wl_ref, sems.at[PIECES + 1]),
        pltpu.make_async_copy(wr_hbm, wr_ref, sems.at[PIECES + 2]),
    ]
    for copy in weights[:1] + pieces + weights[1:]:
        copy.start()
    weights[0].wait()
    gain = gain_ref[...]
    for p in range(PIECES):
        pieces[p].wait()
        x = x_ref[pl.ds(p * part, part)].reshape(part * n, c).astype(F32)
        centred = x - jnp.mean(x, axis=-1, keepdims=True)
        power = jnp.mean(centred * centred, axis=-1, keepdims=True)
        ready = (centred * lax.rsqrt(power + 1e-05) * gain).astype(BF16)
        ready_ref[pl.ds(p * part * n, part * n), :] = ready
        rows = ready.astype(F32)
        for q in range(part):
            rows_ref[pl.ds((p * part + q) * pitch, n), :] = rows[q * n : (q + 1) * n]
    weights[1].wait()
    weights[2].wait()
    w = jnp.concatenate([wl_ref[...].astype(F32).T, wr_ref[...].astype(F32).T], axis=0).astype(BF16)
    for i in range(n):
        both = nt(w, rows_ref[pl.ds(i, k, stride=pitch), :].astype(BF16))
        tiles_ref[pl.ds(i, d, stride=wide), :] = both[:d]
        tiles_ref[pl.ds(n + i, d, stride=wide), :] = both[d:]
    step = 32

    def store(s, _):
        for q in range(step):
            out_ref[s * step + q] = tiles_ref[pl.ds((s * step + q) * wide, 2 * n), :].astype(BF16)
        return 0

    lax.fori_loop(0, d // step, store, 0)


def gate_kernel(ready_ref, gate_hbm, gain_hbm, w_hbm, out_ref, gain_out_ref, w_out_ref, gate_ref, gain_ref, sems):
    copies = [
        pltpu.make_async_copy(gate_hbm, gate_ref, sems.at[0]),
        pltpu.make_async_copy(gain_hbm, gain_ref, sems.at[1]),
        pltpu.make_async_copy(w_hbm, w_out_ref, sems.at[2]),
    ]
    for copy in copies:
        copy.start()
    for copy in copies:
        copy.wait()
    g = gate_ref[...]
    step = 256

    def one(s, _):
        at = pl.ds(s * step, step)
        out_ref[at, :] = jax.nn.sigmoid(jnp.dot(ready_ref[at, :], g, preferred_element_type=F32))
        return 0

    lax.fori_loop(0, ready_ref.shape[0] // step, one, 0)
    gain_out_ref[...] = gain_ref[...]


def middle_kernel(rows, scale, own_ref, other_ref, out_ref):
    chips, per, n, k = other_ref.shape
    halves = rows // 2
    plane = chips // halves
    few = plane // rows
    for dd in range(per):
        right = jnp.concatenate(
            [own_ref[pl.ds(r * plane, plane), dd, n:, :].reshape(plane * n, k) for r in range(halves)], axis=1
        )
        for to in range(rows):
            left = []
            for r in range(halves):
                at = pl.ds(r * plane + to * few, few)
                both = jnp.concatenate(
                    [own_ref[at, dd, :n, :].reshape(few * n, k), other_ref[at, dd].reshape(few * n, k)], axis=0
                )
                left.append(both.astype(F32).T.astype(BF16))
            total = jnp.dot(right, jnp.concatenate(left, axis=0), preferred_element_type=F32) * scale
            out_ref[pl.ds(to * plane, plane), dd] = total.astype(BF16).reshape(plane, n, k)


def back_kernel(m_ref, gate_ref, gain_ref, w_ref, out_hbm, rows_ref, sums_ref, out_ref, sems):
    d2, n, k = m_ref.shape
    d = d2 // 2
    pitch = n + 1
    step = 32

    def total(s, acc):
        for q in range(step):
            at = s * step + q
            m = m_ref[at].astype(F32) + m_ref[d + at].astype(F32)
            rows_ref[pl.ds(at * pitch, n), :] = m
            acc += m
        return acc

    mean = lax.fori_loop(0, d // step, total, jnp.zeros((n, k), F32)) * (1.0 / d)

    def squares(s, acc):
        for q in range(step):
            centred = rows_ref[pl.ds((s * step + q) * pitch, n), :] - mean
            acc += centred * centred
        return acc

    power = lax.fori_loop(0, d // step, squares, jnp.zeros((n, k), F32)) * (1.0 / d)
    root = lax.rsqrt(power + 1e-05)

    def scaled(s, _):
        for q in range(step):
            at = pl.ds((s * step + q) * pitch, n)
            rows_ref[at, :] = (rows_ref[at, :] - mean) * root
        return 0

    lax.fori_loop(0, d // step, scaled, 0)
    w = w_ref[...]
    gain = gain_ref[...]
    core = lax.rem(lax.axis_index("col"), 2)
    for j in range(n):
        t = (rows_ref[pl.ds(j, d, stride=pitch), :].T * gain).astype(BF16)
        sums = jnp.dot(t, w, preferred_element_type=F32)
        for h in range(2):
            for q in range(k // (2 * n)):
                at = (2 * q + (1 - core if h else core)) * n * pitch + j
                block = h * (k // 2) + q * n
                sums_ref[pl.ds(at, n, stride=pitch), :] = sums[block : block + n]
    part = k // PIECES
    copies = []
    for p in range(PIECES):

        def finish(s, _):
            for q in range(step):
                at = p * part + s * step + q
                out_ref[at] = (sums_ref[pl.ds(at * pitch, n), :] * gate_ref[pl.ds(at * n, n), :]).astype(BF16)
            return 0

        lax.fori_loop(0, part // step, finish, 0)
        copy = pltpu.make_async_copy(
            out_ref.at[pl.ds(p * part, part)], out_hbm.at[pl.ds(p * part, part)], sems.at[p]
        )
        copy.start()
        copies.append(copy)
    for copy in copies:
        copy.wait()


def body(pair_array, in_gain, left_weight, right_weight, mid_gain, out_weight, out_gate):
    k, n, c = pair_array.shape
    d = left_weight.shape[1]
    rows, cols = lax.axis_size("row"), lax.axis_size("col")
    params = pltpu.CompilerParams(vmem_limit_bytes=32 << 20)
    ready, factors = pl.pallas_call(
        front_kernel,
        out_shape=(
            jax.ShapeDtypeStruct((k * n, c), BF16),
            jax.ShapeDtypeStruct((d, 2 * n, k), BF16),
        ),
        in_specs=[HBM] * 4,
        out_specs=(VMEM, VMEM),
        scratch_shapes=[
            pltpu.VMEM((k, n, c), BF16),
            pltpu.VMEM((1, c), F32),
            pltpu.VMEM((c, d), BF16),
            pltpu.VMEM((c, d), BF16),
            pltpu.VMEM((k * (n + 1), c), F32),
            pltpu.VMEM((d * (2 * n + 1), k), F32),
            pltpu.SemaphoreType.DMA((PIECES + 3,)),
        ],
        compiler_params=params,
        name="front",
    )(in_hbm(pair_array), in_hbm(in_gain.reshape(1, c)), in_hbm(left_weight), in_hbm(right_weight))
    chips = rows * cols // 2
    every = [[r * cols + q * 2 + core for r in range(rows) for q in range(cols // 2)] for core in range(2)]
    of_half = [group[h * chips // 2 : (h + 1) * chips // 2] for group in every for h in range(2)]
    per = d // (chips // 2)

    def exchange(x, groups):
        return lax.all_to_all(
            x, ("row", "col"), split_axis=0, concat_axis=0, tiled=True, axis_index_groups=groups
        )

    factors = exchange(factors, of_half).reshape(chips // 2, per, 2 * n, k)
    other = lax.ppermute(factors[:, :, :n], "col", [(i, i ^ 1) for i in range(cols)])
    gate, gain, weight = pl.pallas_call(
        gate_kernel,
        out_shape=(
            jax.ShapeDtypeStruct((k * n, c), F32),
            jax.ShapeDtypeStruct((1, d), F32),
            jax.ShapeDtypeStruct((d, c), BF16),
        ),
        in_specs=[VMEM, HBM, HBM, HBM],
        out_specs=(VMEM, VMEM, VMEM),
        scratch_shapes=[
            pltpu.VMEM((c, c), BF16),
            pltpu.VMEM((1, d), F32),
            pltpu.SemaphoreType.DMA((3,)),
        ],
        compiler_params=params,
        cost_estimate=pl.CostEstimate(flops=4_000_000_000, bytes_accessed=2 << 20, transcendentals=k * n * c),
        name="gate",
    )(ready, in_hbm(out_gate), in_hbm(mid_gain.reshape(1, d)), in_hbm(out_weight))
    factors, other, gate, gain, weight = lax.optimization_barrier((factors, other, gate, gain, weight))
    mixed = pl.pallas_call(
        functools.partial(middle_kernel, rows, (k * rows) ** -0.5),
        out_shape=jax.ShapeDtypeStruct((chips, per, n, k), BF16),
        in_specs=[VMEM] * 2,
        out_specs=VMEM,
        compiler_params=params,
        name="middle",
    )(factors, other)
    mixed = exchange(mixed.reshape(2 * d, n, k), every)
    return pl.pallas_call(
        back_kernel,
        out_shape=jax.ShapeDtypeStruct((k, n, c), BF16),
        in_specs=[VMEM] * 4,
        out_specs=HBM,
        scratch_shapes=[
            pltpu.VMEM((d * (n + 1), k), F32),
            pltpu.VMEM((k * (n + 1), c), F32),
            pltpu.VMEM((k, n, c), BF16),
            pltpu.SemaphoreType.DMA((PIECES,)),
        ],
        compiler_params=params,
        name="back",
    )(mixed, gate, gain, weight)


def solution(mesh):
    return jax.shard_map(
        body,
        mesh=mesh,
        in_specs=(
            P(("site", "row"), "col", None),
            P(),
            P("site", None),
            P("site", None),
            P(),
            P("site", None),
            P("site", None),
        ),
        out_specs=P(("site", "row"), "col", None),
        check_vma=False,
    )
```

```python
import functools

import jax
import jax.numpy as jnp
from jax import lax
from jax.experimental import pallas as pl
from jax.experimental.pallas import tpu as pltpu
from jax.sharding import PartitionSpec as P

VMEM = pl.BlockSpec(memory_space=pltpu.VMEM)
HBM = pl.BlockSpec(memory_space=pltpu.HBM)
F32 = jnp.float32
BF16 = jnp.bfloat16
PIECES = 2


def nt(a, b):
    return lax.dot_general(a, b, (((1,), (1,)), ((), ())), preferred_element_type=F32)


def in_hbm(x):
    return pltpu.with_memory_space_constraint(x, pltpu.HBM)


def front_kernel(x_hbm, gain_hbm, wl_hbm, wr_hbm, gate_hbm, mid_gain_hbm, wo_hbm,
                 ready_ref, out_ref, gate_ref, mid_gain_ref, wo_ref,
                 x_ref, gain_ref, wl_ref, wr_ref, rows_ref, tiles_ref, sems):
    k, n, c = x_ref.shape
    d = wl_ref.shape[1]
    pitch, wide = n + 1, 2 * n + 1
    part = k // PIECES
    pieces = [(x_hbm.at[pl.ds(p * part, part)], x_ref.at[pl.ds(p * part, part)]) for p in range(PIECES)]
    weights = [(wl_hbm, wl_ref), (wr_hbm, wr_ref), (gain_hbm, gain_ref)]
    later = [(gate_hbm, gate_ref), (mid_gain_hbm, mid_gain_ref), (wo_hbm, wo_ref)]
    copies = [
        pltpu.make_async_copy(src, dst, sems.at[at]) for at, (src, dst) in enumerate(weights + pieces + later)
    ]
    for copy in copies:
        copy.start()
    for copy in copies[:3]:
        copy.wait()
    w = jnp.concatenate([wl_ref[...].astype(F32).T, wr_ref[...].astype(F32).T], axis=0).astype(BF16)
    gain = gain_ref[...]
    for p in range(PIECES):
        copies[3 + p].wait()
        x = x_ref[pl.ds(p * part, part)].reshape(part * n, c).astype(F32)
        centred = x - jnp.mean(x, axis=-1, keepdims=True)
        power = jnp.mean(centred * centred, axis=-1, keepdims=True)
        ready = (centred * lax.rsqrt(power + 1e-05) * gain).astype(BF16)
        ready_ref[pl.ds(p * part * n, part * n), :] = ready
        rows = ready.astype(F32)
        for q in range(part):
            rows_ref[pl.ds((p * part + q) * pitch, n), :] = rows[q * n : (q + 1) * n]
    for i in range(n):
        both = nt(w, rows_ref[pl.ds(i, k, stride=pitch), :].astype(BF16))
        tiles_ref[pl.ds(i, d, stride=wide), :] = both[:d]
        tiles_ref[pl.ds(n + i, d, stride=wide), :] = both[d:]
    for q in range(d):
        out_ref[q] = tiles_ref[pl.ds(q * wide, 2 * n), :].astype(BF16)
    for copy in copies[3 + PIECES :]:
        copy.wait()


def gate_kernel(ready_ref, gate_ref, out_ref):
    out_ref[...] = jax.nn.sigmoid(jnp.dot(ready_ref[...], gate_ref[...], preferred_element_type=F32))


def middle_kernel(rows, scale, own_ref, other_ref, out_ref):
    chips, per, n, k = other_ref.shape
    halves = rows // 2
    plane = chips // halves
    few = plane // rows
    for dd in range(per):
        right = jnp.concatenate(
            [own_ref[pl.ds(r * plane, plane), dd, n:, :].reshape(plane * n, k) for r in range(halves)], axis=1
        )
        lines = []
        for to in range(rows):
            left = []
            for r in range(halves):
                at = pl.ds(r * plane + to * few, few)
                both = jnp.concatenate(
                    [own_ref[at, dd, :n, :].reshape(few * n, k), other_ref[at, dd].reshape(few * n, k)], axis=0
                )
                left.append(both.T)
            lines.append(jnp.concatenate(left, axis=0))
        for to in range(0, rows, 2):
            total = jnp.dot(right, jnp.concatenate(lines[to : to + 2], axis=1), preferred_element_type=F32) * scale
            for q in range(2):
                tile = total[:, q * k : (q + 1) * k].astype(BF16).reshape(plane, n, k)
                out_ref[pl.ds((to + q) * plane, plane), dd] = tile


def back_kernel(m_ref, gate_ref, gain_ref, w_ref, out_hbm, rows_ref, sums_ref, out_ref, sems):
    d2, n, k = m_ref.shape
    d = d2 // 2
    pitch = n + 1
    def over_channels(term):
        parts = [jnp.zeros((n, k), F32) for _ in range(4)]
        for at in range(d):
            parts[at % 4] += term(at)
        return (parts[0] + parts[1]) + (parts[2] + parts[3])

    def value(at):
        m = m_ref[at].astype(F32) + m_ref[d + at].astype(F32)
        rows_ref[pl.ds(at * pitch, n), :] = m
        return m

    mean = over_channels(value) * (1.0 / d)

    def square(at):
        centred = rows_ref[pl.ds(at * pitch, n), :] - mean
        return centred * centred

    root = lax.rsqrt(over_channels(square) * (1.0 / d) + 1e-05)
    for at in range(d):
        line = pl.ds(at * pitch, n)
        rows_ref[line, :] = (rows_ref[line, :] - mean) * root
    w = w_ref[...]
    gain = gain_ref[...]
    core = lax.rem(lax.axis_index("col"), 2)
    for j in range(n):
        t = (rows_ref[pl.ds(j, d, stride=pitch), :].T * gain).astype(BF16)
        sums = jnp.dot(t, w, preferred_element_type=F32)
        for h in range(2):
            for q in range(k // (2 * n)):
                at = (2 * q + (1 - core if h else core)) * n * pitch + j
                block = h * (k // 2) + q * n
                sums_ref[pl.ds(at, n, stride=pitch), :] = sums[block : block + n]
    part = k // PIECES
    copies = []
    for p in range(PIECES):
        for at in range(p * part, (p + 1) * part):
            out_ref[at] = (sums_ref[pl.ds(at * pitch, n), :] * gate_ref[pl.ds(at * n, n), :]).astype(BF16)
        copy = pltpu.make_async_copy(
            out_ref.at[pl.ds(p * part, part)], out_hbm.at[pl.ds(p * part, part)], sems.at[p]
        )
        copy.start()
        copies.append(copy)
    for copy in copies:
        copy.wait()


def body(pair_array, in_gain, left_weight, right_weight, mid_gain, out_weight, out_gate):
    k, n, c = pair_array.shape
    d = left_weight.shape[1]
    rows, cols = lax.axis_size("row"), lax.axis_size("col")
    params = pltpu.CompilerParams(vmem_limit_bytes=32 << 20)
    ready, factors, gate_weight, gain, weight = pl.pallas_call(
        front_kernel,
        out_shape=(
            jax.ShapeDtypeStruct((k * n, c), BF16),
            jax.ShapeDtypeStruct((d, 2 * n, k), BF16),
            jax.ShapeDtypeStruct((c, c), BF16),
            jax.ShapeDtypeStruct((1, d), F32),
            jax.ShapeDtypeStruct((d, c), BF16),
        ),
        in_specs=[HBM] * 7,
        out_specs=(VMEM,) * 5,
        scratch_shapes=[
            pltpu.VMEM((k, n, c), BF16),
            pltpu.VMEM((1, c), F32),
            pltpu.VMEM((c, d), BF16),
            pltpu.VMEM((c, d), BF16),
            pltpu.VMEM((k * (n + 1), c), F32),
            pltpu.VMEM((d * (2 * n + 1), k), F32),
            pltpu.SemaphoreType.DMA((PIECES + 6,)),
        ],
        compiler_params=params,
        name="front",
    )(
        in_hbm(pair_array),
        in_hbm(in_gain.reshape(1, c)),
        in_hbm(left_weight),
        in_hbm(right_weight),
        in_hbm(out_gate),
        in_hbm(mid_gain.reshape(1, d)),
        in_hbm(out_weight),
    )
    chips = rows * cols // 2
    every = [[r * cols + q * 2 + core for r in range(rows) for q in range(cols // 2)] for core in range(2)]
    of_half = [group[h * chips // 2 : (h + 1) * chips // 2] for group in every for h in range(2)]
    per = d // (chips // 2)

    def exchange(x, groups):
        return lax.all_to_all(
            x, ("row", "col"), split_axis=0, concat_axis=0, tiled=True, axis_index_groups=groups
        )

    factors = exchange(factors, of_half).reshape(chips // 2, per, 2 * n, k)
    other = lax.ppermute(factors[:, :, :n], "col", [(i, i ^ 1) for i in range(cols)])
    gate = pl.pallas_call(
        gate_kernel,
        out_shape=jax.ShapeDtypeStruct((k * n, c), F32),
        in_specs=[VMEM] * 2,
        out_specs=VMEM,
        compiler_params=params,
        cost_estimate=pl.CostEstimate(flops=4_000_000_000, bytes_accessed=2 << 20, transcendentals=k * n * c),
        name="gate",
    )(ready, gate_weight)
    factors, other, gate = lax.optimization_barrier((factors, other, gate))
    mixed = pl.pallas_call(
        functools.partial(middle_kernel, rows, (k * rows) ** -0.5),
        out_shape=jax.ShapeDtypeStruct((chips, per, n, k), BF16),
        in_specs=[VMEM] * 2,
        out_specs=VMEM,
        compiler_params=params,
        name="middle",
    )(factors, other)
    mixed = exchange(mixed.reshape(2 * d, n, k), every)
    return pl.pallas_call(
        back_kernel,
        out_shape=jax.ShapeDtypeStruct((k, n, c), BF16),
        in_specs=[VMEM] * 4,
        out_specs=HBM,
        scratch_shapes=[
            pltpu.VMEM((d * (n + 1), k), F32),
            pltpu.VMEM((k * (n + 1), c), F32),
            pltpu.VMEM((k, n, c), BF16),
            pltpu.SemaphoreType.DMA((PIECES,)),
        ],
        compiler_params=params,
        name="back",
    )(mixed, gate, gain, weight)


def solution(mesh):
    return jax.shard_map(
        body,
        mesh=mesh,
        in_specs=(
            P(("site", "row"), "col", None),
            P(),
            P("site", None),
            P("site", None),
            P(),
            P("site", None),
            P("site", None),
        ),
        out_specs=P(("site", "row"), "col", None),
        check_vma=False,
    )
```
